512 devices in a mesh: sector: 64 (over x, z_lo, y), block: 8 (over z_hi, core).
Axes of the slice: x: 4, y: 8, z: 8 (z_hi: 4, z_lo: 2; z = z_hi * 2 + z_lo), core: 2. Of those that a mesh axis runs over, the one named last changes fastest.
Arguments:
- adjoint_prev: float32 [5, 64, 512, 128], P(None, 'block', 'sector'), may hold values from -6 to 6
- adjoint_source: float32 [5, 64, 512, 128], P(None, 'block', 'sector'), may hold values from -6 to 6
- face_matrices: bfloat16 [3, 5, 5, 64, 512, 128], P(None, None, None, 'block', 'sector'), may hold values from -2.5 to 2.5
- inverse_blocks: bfloat16 [5, 5, 64, 512, 128], P(None, None, 'block', 'sector')
- sector_offset: int32 [1], replicated, may hold values from 1 to 63
- donor_cells: int32 [512], P('sector'), may hold values from 0 to 7
- donor_weights: float32 [512], P('sector'), may hold values from 0.1 to 0.9
Outputs:
- adjoint: float32 [5, 64, 512, 128], P(None, 'block', 'sector')
- last_update: float32 [5, 64, 512, 128], P(None, 'block', 'sector')
The draws below stay inside these ranges and needn't reach their ends.
All inputs are finite; a program needn't handle non-finite values.
Results may differ from the reference program's by a relative error of at most 0.0003.
Values sent between devices are 32-bit elements; how exact they have to be, the bound alone decides.
A program may use at most 64 MiB of HBM per device.

```python
import jax
import jax.numpy as jnp

CT = 8
NRAD = 128
ITERS = 4
NAX = 64
NCIRC = 512
N_SECTOR = 64


def draw_inverse_blocks(key, part):
    key_off = jax.random.fold_in(key, 11)
    key_diag = jax.random.fold_in(key, 12)
    off_part = 0.06 * jax.random.normal(key_off, (5, 5, NAX, NCIRC, NRAD), jnp.float32)
    diag_part = jnp.exp(jax.random.uniform(key_diag, (5, NAX, NCIRC, NRAD), jnp.float32, jnp.log(0.15), jnp.log(0.3)))
    identity = jnp.eye(5, dtype=jnp.float32)[:, :, None, None, None]
    return (off_part * (1.0 - identity) + identity * diag_part[:, None]).astype(jnp.bfloat16)


def touch_ends(values, key, least, largest):
    longest = values.shape.index(max(values.shape))
    spots = []
    for shift in (0, 1):
        where = [jax.random.randint(jax.random.fold_in(key, axis), (), 0, length) for axis, length in enumerate(values.shape)]
        where[longest] = (where[longest] + shift) % values.shape[longest]
        spots.append(tuple(where))
    return values.at[spots[0]].set(least).at[spots[1]].set(largest)


def block_scale(rng, shape, pieces, low, largest):
    loudness = 1.0
    for dim, blocks in pieces:
        steps = jax.random.uniform(jax.random.fold_in(jax.random.fold_in(rng, 6), dim), (blocks,), jnp.float32, low / len(pieces), largest / len(pieces))
        loudness = loudness * jnp.repeat(jnp.exp(steps), shape[dim] // blocks).reshape((-1,) + (1,) * (len(shape) - 1 - dim))
    return loudness


def scatter_about(key, extent, deviation, reach, shards=(), kind=jnp.bfloat16):
    factor_of = block_scale(key, extent, shards, -0.22, 0.18) if shards else 1.0
    array = jax.random.normal(key, extent, jnp.float32) * deviation * factor_of
    return jnp.minimum(jnp.maximum(array, -reach), reach).astype(kind)


def setup_inputs(seed: int = 0) -> dict:
    streams_of = jax.random.split(jax.random.key(seed), 8)
    return {
        "adjoint_prev": scatter_about(streams_of[0], (5, NAX, NCIRC, NRAD), 1.0, 6.0, ((1, 8), (2, 64)), jnp.float32),
        "adjoint_source": scatter_about(streams_of[1], (5, NAX, NCIRC, NRAD), 1.0, 6.0, ((1, 8), (2, 64)), jnp.float32),
        "face_matrices": scatter_about(streams_of[2], (3, 5, 5, NAX, NCIRC, NRAD), 5 ** -0.5, 2.5, ((3, 8), (4, 64))),
        "inverse_blocks": draw_inverse_blocks(jax.random.fold_in(streams_of[7], 71), 0),
        "sector_offset": jax.random.randint(streams_of[4], (1,), 1, N_SECTOR).astype(jnp.int32),
        "donor_cells": touch_ends(jax.random.randint(streams_of[5], (NCIRC,), 0, CT), jax.random.fold_in(streams_of[5], 1), 0, CT - 1).astype(jnp.int32),
        "donor_weights": jnp.clip(0.1 + 0.79999997 * jax.random.uniform(streams_of[6], (NCIRC,), jnp.float32) ** block_scale(streams_of[6], (NCIRC,), ((0, 64),), -0.2, 0.2), 0.1, 0.9),
    }


def neighbour_terms(adjoint, sector_offset, donor_cells, donor_weights):
    first = NAX // 2
    rotor_row = adjoint[:, first - 1]
    shift_cells = sector_offset[0] * CT
    base = (jnp.arange(NCIRC, dtype=jnp.int32) // CT) * CT + donor_cells
    source_one = jnp.mod(base - shift_cells, NCIRC).astype(jnp.int32)
    source_two = jnp.mod(base + 1 - shift_cells, NCIRC).astype(jnp.int32)
    weights = donor_weights[None, :, None]
    facing = weights * jnp.take(rotor_row, source_one, axis=1) + (1.0 - weights) * jnp.take(rotor_row, source_two, axis=1)
    zero_layer = jnp.zeros_like(adjoint[:, :1])
    axial_minus = jnp.concatenate([zero_layer, adjoint[:, :-1]], axis=1)
    axial_minus = axial_minus.at[:, first].set(facing)
    axial_plus = jnp.concatenate([adjoint[:, 1:], zero_layer], axis=1)
    around_minus = jnp.roll(adjoint, 1, axis=2)
    around_plus = jnp.roll(adjoint, -1, axis=2)
    padded = jnp.pad(adjoint, ((0, 0), (0, 0), (0, 0), (1, 1)))
    radial_minus = padded[:, :, :, :-2]
    radial_plus = padded[:, :, :, 2:]
    return (0.6 * axial_minus + 0.4 * axial_plus,
            0.6 * around_minus + 0.4 * around_plus,
            0.6 * radial_minus + 0.4 * radial_plus)


def sweep(adjoint, adjoint_source, face_matrices, inverse_blocks, sector_offset, donor_cells, donor_weights):
    mixed = neighbour_terms(adjoint, sector_offset, donor_cells, donor_weights)
    coupled = jnp.zeros_like(adjoint)
    for direction in range(3):
        for comp in range(5):
            coupled = coupled + face_matrices[direction, comp].astype(jnp.float32) * mixed[direction][comp][None]
    total = adjoint_source + coupled
    result = jnp.zeros_like(adjoint)
    for comp in range(5):
        result = result + inverse_blocks[:, comp].astype(jnp.float32) * total[comp][None]
    return result


def reference(adjoint_prev, adjoint_source, face_matrices, inverse_blocks, sector_offset, donor_cells, donor_weights):
    adjoint = adjoint_prev
    last_update = jnp.zeros_like(adjoint_prev)
    for sweep_number in range(ITERS):
        result = sweep(adjoint, adjoint_source, face_matrices, inverse_blocks, sector_offset, donor_cells, donor_weights)
        last_update = result - adjoint
        adjoint = result
    return adjoint, last_update
```

```python
import functools

import jax
import jax.numpy as jnp
from jax import lax
from jax.experimental import pallas as pl
from jax.experimental.pallas import tpu as pltpu
from jax.sharding import PartitionSpec as P

ITERS = 4
MESH = pl.DeviceIdType.MESH
LEFT, RIGHT, DOWN, UP = range(4)


def radices(sectors):
    return (sectors // 16, 2, 8) if sectors >= 16 else (2, 2, 2)


def kernel(
    sectors,
    blocks,
    prev_ref,
    source_ref,
    faces_ref,
    inverse_ref,
    offset_ref,
    cells_ref,
    weights_ref,
    out_ref,
    update_ref,
    field,
    partial,
    source,
    faces_narrow,
    inverse_narrow,
    faces,
    inverse,
    first_columns,
    last_columns,
    from_left,
    from_right,
    from_below,
    from_above,
    slots_y,
    message_x,
    slots_x,
    message_z,
    slots_z,
    load_sems,
    send_sems,
    recv_sems,
    send_y,
    recv_y,
    send_x,
    recv_x,
    send_z,
    recv_z,
):
    layers, around, radial = prev_ref.shape[1:]
    across, deep, along = radices(sectors)
    group = deep * along
    sector = lax.axis_index("sector")
    block = lax.axis_index("block")
    at_x = sector // group
    at_z = lax.rem(sector // along, deep)
    at_y = lax.rem(sector, along)
    left = lax.rem(sector + sectors - 1, sectors)
    right = lax.rem(sector + 1, sectors)
    is_facing = block == blocks // 2 - 1
    is_faced = block == blocks // 2
    has_above = block < blocks - 1
    has_below = block > 0

    def place(x, z, y):
        return x * group + z * along + y

    def moved_y(distance):
        return place(at_x, at_z, lax.rem(at_y + distance + along, along))

    def moved_x(distance):
        return place(lax.rem(at_x + distance + across, across), at_z, at_y)

    def moved_z(distance):
        return place(at_x, lax.rem(at_z + distance + deep, deep), at_y)

    barrier = pltpu.get_barrier_semaphore()

    def greet(to_sector, to_block):
        pl.semaphore_signal(barrier, inc=1, device_id=(to_sector, to_block), device_id_type=MESH)

    @pl.when(is_faced)
    def _():
        for distance in range(deep):
            greet(moved_z(-distance), block - 1)

    @pl.when(is_facing)
    def _():
        for distance in range(1, along):
            greet(moved_y(-distance), block)
        for distance in range(1, across):
            greet(moved_x(-distance), block)

    greet(left, block)
    greet(right, block)

    @pl.when(has_above)
    def _():
        greet(sector, block + 1)

    @pl.when(jnp.logical_and(has_below, jnp.logical_not(is_faced)))
    def _():
        greet(sector, block - 1)

    def load(index, src, dst):
        return pltpu.make_async_copy(src, dst, load_sems.at[index])

    load_prev = load(0, prev_ref, field.at[0, :, pl.ds(1, layers)])
    load_source = load(1, source_ref, source)
    load_faces = load(2, faces_ref, faces_narrow)
    load_inverse = load(3, inverse_ref, inverse_narrow)
    load_prev.start()
    load_faces.start()
    load_inverse.start()
    load_source.start()

    def remote(src, dst, send_sem, recv_sem, to_sector, to_block):
        return pltpu.make_async_remote_copy(
            src_ref=src,
            dst_ref=dst,
            send_sem=send_sem,
            recv_sem=recv_sem,
            device_id=(to_sector, to_block),
            device_id_type=MESH,
        )

    def step_copy(k, direction, src, dst, to_sector, to_block):
        return remote(src, dst, send_sems.at[k, direction], recv_sems.at[k, direction], to_sector, to_block)

    def to_left(k):
        return step_copy(k, LEFT, first_columns.at[k], from_right.at[k], left, block)

    def to_right(k):
        return step_copy(k, RIGHT, last_columns.at[k], from_left.at[k], right, block)

    def downward(k):
        return step_copy(k, DOWN, field.at[k, :, 1], from_above.at[k], sector, block - 1)

    def upward(k):
        return step_copy(k, UP, field.at[k, :, layers], from_below.at[k], sector, block + 1)

    def row_y(k, distance):
        return remote(
            field.at[k, :, layers],
            slots_y.at[k, distance],
            send_y.at[k, distance],
            recv_y.at[k, distance],
            moved_y(distance),
            block,
        )

    def row_x(k, distance):
        return remote(
            message_x.at[k],
            slots_x.at[k, distance],
            send_x.at[k, distance],
            recv_x.at[k, distance],
            moved_x(distance),
            block,
        )

    def row_z(k, distance):
        return remote(
            message_z.at[k],
            slots_z.at[k, distance],
            send_z.at[k, distance],
            recv_z.at[k, distance],
            moved_z(distance),
            block + 1,
        )

    def path(offset):
        back_y = lax.rem(offset, along)
        rest = offset // along + (at_y < back_y).astype(jnp.int32)
        back_z = lax.rem(rest, deep)
        return back_y, rest // deep, back_z

    row_path = path(offset_ref[0])
    column_path = path(offset_ref[0] - 1)

    def slot_x(whole):
        _, back_x, back_z = whole
        return lax.rem(back_x + (at_z + back_z >= deep).astype(jnp.int32), across)

    nothing = jnp.zeros((5, around, radial), jnp.float32)

    def clear(k, carry):
        field[k, :, 0] = nothing
        field[k, :, layers + 1] = nothing

        @pl.when(jnp.logical_not(has_below))
        def _():
            from_below[k] = nothing

        @pl.when(jnp.logical_not(has_above))
        def _():
            from_above[k] = nothing

        @pl.when(is_facing)
        def _():
            message_x[k, 5] = jnp.zeros((around, radial), jnp.float32)

        return carry

    lax.fori_loop(0, ITERS, clear, 0)

    def masks(count):
        shape = (count, around, radial)
        rows = lax.broadcasted_iota(jnp.int32, shape, 1)
        lanes = lax.broadcasted_iota(jnp.int32, shape, 2)
        return rows == 0, rows == around - 1, lanes == 0, lanes == radial - 1

    def pack(k, some, value):
        first_columns[k, :, some] = value[:, :, 0:1]
        last_columns[k, :, some] = value[:, :, around - 1 : around]

    def send(k):
        @pl.when(is_facing)
        def _():
            for distance in range(1, along):
                row_y(k, distance).start()
            slots_y[k, 0] = field[k, :, layers]

        @pl.when(jnp.logical_and(has_above, jnp.logical_not(is_facing)))
        def _():
            upward(k).start()

        @pl.when(has_below)
        def _():
            downward(k).start()

        to_left(k).start()
        to_right(k).start()

    def pick(index, choices):
        value = choices[0]
        wanted = jnp.broadcast_to(index, value.shape)
        for place_back in range(1, len(choices)):
            value = jnp.where(wanted == place_back, choices[place_back], value)
        return value

    def turn_x(k):
        for distance in range(1, along):
            row_y(k, distance).wait_recv()
        message_x[k, pl.ds(0, 5)] = pick(row_path[0], [slots_y[k, back] for back in range(along)])
        message_x[k, 5, pl.ds(0, 5)] = pick(
            column_path[0], [slots_y[k, back, :, 0] for back in range(along)]
        )
        for distance in range(1, across):
            row_x(k, distance).start()
        slots_x[k, 0] = message_x[k]

    def turn_z(k):
        for distance in range(1, across):
            row_x(k, distance).wait_recv()
        message_z[k, pl.ds(0, 5)] = pick(
            slot_x(row_path), [slots_x[k, back, pl.ds(0, 5)] for back in range(across)]
        )
        message_z[k, 5] = pick(slot_x(column_path), [slots_x[k, back, 5] for back in range(across)])
        for distance in range(deep):
            row_z(k, distance).start()

    def receive_axial(k):
        @pl.when(has_above)
        def _():
            downward(k).wait_recv()

        @pl.when(jnp.logical_and(has_below, jnp.logical_not(is_faced)))
        def _():
            upward(k).wait_recv()

        @pl.when(is_faced)
        def _():
            for distance in range(deep):
                row_z(k, distance).wait_recv()
            blend_facing(k)

    def blend_facing(k):
        rows = lax.broadcasted_iota(jnp.int32, (around, radial), 0)
        donors = jnp.zeros((around, radial), jnp.int32)
        shares = jnp.zeros((around, radial), jnp.float32)
        for cell in range(around):
            donors = jnp.where(rows == cell, cells_ref[cell], donors)
            shares = jnp.where(rows == cell, weights_ref[cell], shares)
        facing = pick(row_path[2], [slots_z[k, back, pl.ds(0, 5)] for back in range(deep)])
        extra = pick(column_path[2], [slots_z[k, back, 5] for back in range(deep)])
        blended = nothing
        for column in range(around + 1):
            share = jnp.where(donors == column, shares, jnp.where(donors == column - 1, 1.0 - shares, 0.0))
            if column < around:
                row = facing[:, column : column + 1]
            else:
                row = jnp.stack([extra[comp : comp + 1] for comp in range(5)])
            blended = blended + share[None] * jnp.broadcast_to(row, (5, around, radial))
        from_below[k] = blended

    def begin(k, low, count):
        some = pl.ds(low, count)
        top, bottom, hub, shroud = masks(count)
        total = source[:, some]
        for comp in range(5):
            here = field[k, comp, pl.ds(low + 1, count)]
            mixed = (
                0.6 * field[k, comp, some] + 0.4 * field[k, comp, pl.ds(low + 2, count)],
                0.6 * jnp.where(top, 0.0, pltpu.roll(here, 1, 1))
                + 0.4 * jnp.where(bottom, 0.0, pltpu.roll(here, around - 1, 1)),
                0.6 * jnp.where(hub, 0.0, pltpu.roll(here, 1, 2))
                + 0.4 * jnp.where(shroud, 0.0, pltpu.roll(here, radial - 1, 2)),
            )
            for direction in range(3):
                total = total + faces[direction, comp, :, some] * mixed[direction][None]
        partial[:, some] = total

    def add_axial(k, layer, share, halo):
        total = partial[:, layer]
        for comp in range(5):
            total = total + faces[0, comp, :, layer] * (share * halo[k, comp])[None]
        partial[:, layer] = total

    def finish(k, low, count):
        some = pl.ds(low, count)
        top, bottom, _, _ = masks(count)
        total = partial[:, some]
        for comp in range(5):
            behind = jnp.broadcast_to(0.6 * from_left[k, comp, some], (count, around, radial))
            ahead = jnp.broadcast_to(0.4 * from_right[k, comp, some], (count, around, radial))
            mixed = jnp.where(top, behind, jnp.where(bottom, ahead, 0.0))
            total = total + faces[1, comp, :, some] * mixed[None]
        value = inverse[0, :, some] * total[0][None]
        for comp in range(1, 5):
            value = value + inverse[comp, :, some] * total[comp][None]
        field[k + 1, :, pl.ds(low + 1, count)] = value
        pack(k + 1, some, value)

    load_prev.wait()
    pack(0, pl.ds(0, layers), field[0, :, pl.ds(1, layers)])

    ends = jnp.logical_or(block == 0, block == blocks - 1)
    ends_extra = 0 if blocks > 2 else -1

    @pl.when(is_facing)
    def _():
        pl.semaphore_wait(barrier, 3 + ends_extra + (along - 1) + (across - 1) + deep)

    @pl.when(jnp.logical_and(ends, jnp.logical_not(is_facing)))
    def _():
        pl.semaphore_wait(barrier, 3)

    @pl.when(jnp.logical_not(jnp.logical_or(ends, is_facing)))
    def _():
        pl.semaphore_wait(barrier, 4)

    half = layers // 2
    inner = half - 1

    def widen_faces(index, carry):
        direction, comp = index // 5, lax.rem(index, 5)
        faces[direction, comp] = faces_narrow[direction, comp].astype(jnp.float32)
        return carry

    def widen_inverse(index, carry):
        onto, comp = index // 5, lax.rem(index, 5)
        inverse[comp, onto] = inverse_narrow[onto, comp].astype(jnp.float32)
        return carry

    def sweep(k, carry):
        send(k)

        @pl.when(k == 0)
        def _():
            load_faces.wait()
            load_inverse.wait()
            lax.fori_loop(0, 15, widen_faces, 0)
            lax.fori_loop(0, 25, widen_inverse, 0)
            load_source.wait()

        @pl.when(jnp.logical_and(is_facing, lax.rem(k, 2) == 1))
        def _():
            turn_x(k - 1)
            turn_x(k)
            turn_z(k - 1)
            turn_z(k)

        begin(k, 0, half)
        begin(k, half, half)
        to_left(k).wait_recv()
        to_right(k).wait_recv()
        finish(k, 1, inner)
        finish(k, half, inner)
        receive_axial(k)
        add_axial(k, 0, 0.6, from_below)
        add_axial(k, layers - 1, 0.4, from_above)
        finish(k, 0, 1)
        finish(k, layers - 1, 1)
        return carry

    lax.fori_loop(0, ITERS, sweep, 0)
    result = field[ITERS, :, pl.ds(1, layers)]
    out_ref[...] = result
    update_ref[...] = result - field[ITERS - 1, :, pl.ds(1, layers)]

    def settle(k, carry):
        to_left(k).wait_send()
        to_right(k).wait_send()

        @pl.when(has_below)
        def _():
            downward(k).wait_send()

        @pl.when(jnp.logical_and(has_above, jnp.logical_not(is_facing)))
        def _():
            upward(k).wait_send()

        @pl.when(is_facing)
        def _():
            for distance in range(1, along):
                row_y(k, distance).wait_send()
            for distance in range(1, across):
                row_x(k, distance).wait_send()
            for distance in range(deep):
                row_z(k, distance).wait_send()

        return carry

    lax.fori_loop(0, ITERS, settle, 0)


def swept(sectors, blocks, *args):
    layers, around, radial = args[0].shape[1:]
    across, deep, along = radices(sectors)
    f32 = jnp.float32
    cells = (5, layers, around, radial)
    anywhere = pl.BlockSpec(memory_space=pl.ANY)
    scalars = pl.BlockSpec(memory_space=pltpu.SMEM)
    vmem = pl.BlockSpec(memory_space=pltpu.VMEM)
    dma = pltpu.SemaphoreType.DMA
    return pl.pallas_call(
        functools.partial(kernel, sectors, blocks),
        out_shape=[OUT(cells, f32)] * 2,
        in_specs=[anywhere] * 4 + [scalars] * 3,
        out_specs=[vmem] * 2,
        scratch_shapes=[
            pltpu.VMEM((ITERS + 1, 5, layers + 2, around, radial), f32),
            pltpu.VMEM(cells, f32),
            pltpu.VMEM(cells, f32),
            pltpu.VMEM((3, 5, 5, layers, around, radial), jnp.bfloat16),
            pltpu.VMEM((5, 5, layers, around, radial), jnp.bfloat16),
            pltpu.VMEM((3, 5, 5, layers, around, radial), f32),
            pltpu.VMEM((5, 5, layers, around, radial), f32),
            pltpu.VMEM((ITERS + 1, 5, layers, 1, radial), f32),
            pltpu.VMEM((ITERS + 1, 5, layers, 1, radial), f32),
            pltpu.VMEM((ITERS, 5, layers, 1, radial), f32),
            pltpu.VMEM((ITERS, 5, layers, 1, radial), f32),
            pltpu.VMEM((ITERS, 5, around, radial), f32),
            pltpu.VMEM((ITERS, 5, around, radial), f32),
            pltpu.VMEM((ITERS, along, 5, around, radial), f32),
            pltpu.VMEM((ITERS, 6, around, radial), f32),
            pltpu.VMEM((ITERS, across, 6, around, radial), f32),
            pltpu.VMEM((ITERS, 6, around, radial), f32),
            pltpu.VMEM((ITERS, deep, 6, around, radial), f32),
            dma((4,)),
            dma((ITERS, 4)),
            dma((ITERS, 4)),
            dma((ITERS, along)),
            dma((ITERS, along)),
            dma((ITERS, across)),
            dma((ITERS, across)),
            dma((ITERS, deep)),
            dma((ITERS, deep)),
        ],
        compiler_params=pltpu.CompilerParams(collective_id=0, has_side_effects=True),
        name="sweeps",
    )(*args)


OUT = pltpu.VMEM


def put_kernel(first_ref, second_ref, first_out, second_out, sems):
    copies = (
        pltpu.make_async_copy(first_ref, first_out, sems.at[0]),
        pltpu.make_async_copy(second_ref, second_out, sems.at[1]),
    )
    for copy in copies:
        copy.start()
    for copy in copies:
        copy.wait()


def put(*values):
    anywhere = pl.BlockSpec(memory_space=pl.ANY)
    return pl.pallas_call(
        put_kernel,
        out_shape=[jax.ShapeDtypeStruct(value.shape, value.dtype) for value in values],
        in_specs=[anywhere] * 2,
        out_specs=[anywhere] * 2,
        scratch_shapes=[pltpu.SemaphoreType.DMA((2,))],
        name="put",
    )(*values)


def shards(prev, source, faces, inverse, sector_offset, donor_cells, donor_weights):
    result = swept(
        lax.axis_size("sector"),
        lax.axis_size("block"),
        prev,
        source,
        faces,
        inverse,
        sector_offset,
        donor_cells,
        donor_weights,
    )
    return tuple(result)


def solution(mesh):
    return jax.shard_map(
        shards,
        mesh=mesh,
        in_specs=(
            P(None, "block", "sector", None),
            P(None, "block", "sector", None),
            P(None, None, None, "block", "sector", None),
            P(None, None, "block", "sector", None),
            P(),
            P("sector"),
            P("sector"),
        ),
        out_specs=(P(None, "block", "sector", None), P(None, "block", "sector", None)),
        check_vma=False,
    )
```

```python
import functools

import jax
import jax.numpy as jnp
from jax import lax
from jax.experimental import pallas as pl
from jax.experimental.pallas import tpu as pltpu
from jax.sharding import PartitionSpec as P

ITERS = 4
MESH = pl.DeviceIdType.MESH
LEFT, RIGHT, DOWN, UP = range(4)


def radices(sectors):
    return (sectors // 16, 2, 8) if sectors >= 16 else (2, 2, 2)


def kernel(
    sectors,
    blocks,
    prev_ref,
    source_ref,
    faces_ref,
    inverse_ref,
    offset_ref,
    cells_ref,
    weights_ref,
    out_ref,
    update_ref,
    field,
    partial,
    source,
    faces_narrow,
    inverse_narrow,
    faces,
    inverse,
    first_columns,
    last_columns,
    from_left,
    from_right,
    from_below,
    from_above,
    slots_y,
    message_x,
    slots_x,
    message_z,
    slots_z,
    load_sems,
    send_sems,
    recv_sems,
    send_y,
    recv_y,
    send_x,
    recv_x,
    send_z,
    recv_z,
):
    layers, around, radial = prev_ref.shape[1:]
    across, deep, along = radices(sectors)
    group = deep * along
    sector = lax.axis_index("sector")
    block = lax.axis_index("block")
    at_x = sector // group
    at_z = lax.rem(sector // along, deep)
    at_y = lax.rem(sector, along)
    left = lax.rem(sector + sectors - 1, sectors)
    right = lax.rem(sector + 1, sectors)
    is_facing = block == blocks // 2 - 1
    is_faced = block == blocks // 2
    has_above = block < blocks - 1
    has_below = block > 0

    def place(x, z, y):
        return x * group + z * along + y

    def moved_y(distance):
        return place(at_x, at_z, lax.rem(at_y + distance + along, along))

    def moved_x(distance):
        return place(lax.rem(at_x + distance + across, across), at_z, at_y)

    def moved_z(distance):
        return place(at_x, lax.rem(at_z + distance + deep, deep), at_y)

    barrier = pltpu.get_barrier_semaphore()

    def greet(to_sector, to_block):
        pl.semaphore_signal(barrier, inc=1, device_id=(to_sector, to_block), device_id_type=MESH)

    @pl.when(is_faced)
    def _():
        for distance in range(deep):
            greet(moved_z(-distance), block - 1)

    @pl.when(is_facing)
    def _():
        for distance in range(1, along):
            greet(moved_y(-distance), block)
        for distance in range(1, across):
            greet(moved_x(-distance), block)

    greet(left, block)
    greet(right, block)

    @pl.when(has_above)
    def _():
        greet(sector, block + 1)

    @pl.when(jnp.logical_and(has_below, jnp.logical_not(is_faced)))
    def _():
        greet(sector, block - 1)

    def load(index, src, dst):
        return pltpu.make_async_copy(src, dst, load_sems.at[index])

    load_prev = load(0, prev_ref, field.at[0, :, pl.ds(1, layers)])
    load_source = load(1, source_ref, source)
    load_faces = load(2, faces_ref, faces_narrow)
    load_inverse = load(3, inverse_ref, inverse_narrow)
    load_prev.start()
    load_faces.start()
    load_inverse.start()
    load_source.start()

    def remote(src, dst, send_sem, recv_sem, to_sector, to_block):
        return pltpu.make_async_remote_copy(
            src_ref=src,
            dst_ref=dst,
            send_sem=send_sem,
            recv_sem=recv_sem,
            device_id=(to_sector, to_block),
            device_id_type=MESH,
        )

    def step_copy(k, direction, src, dst, to_sector, to_block):
        return remote(src, dst, send_sems.at[k, direction], recv_sems.at[k, direction], to_sector, to_block)

    def to_left(k):
        return step_copy(k, LEFT, first_columns.at[k], from_right.at[k], left, block)

    def to_right(k):
        return step_copy(k, RIGHT, last_columns.at[k], from_left.at[k], right, block)

    def downward(k):
        return step_copy(k, DOWN, field.at[k, :, 1], from_above.at[k], sector, block - 1)

    def upward(k):
        return step_copy(k, UP, field.at[k, :, layers], from_below.at[k], sector, block + 1)

    def row_y(k, distance):
        return remote(
            field.at[k, :, layers],
            slots_y.at[k, distance],
            send_y.at[k, distance],
            recv_y.at[k, distance],
            moved_y(distance),
            block,
        )

    def row_x(k, distance):
        return remote(
            message_x.at[k],
            slots_x.at[k, distance],
            send_x.at[k, distance],
            recv_x.at[k, distance],
            moved_x(distance),
            block,
        )

    def row_z(k, distance):
        return remote(
            message_z.at[k],
            slots_z.at[k, distance],
            send_z.at[k, distance],
            recv_z.at[k, distance],
            moved_z(distance),
            block + 1,
        )

    def path(offset):
        back_y = lax.rem(offset, along)
        rest = offset // along + (at_y < back_y).astype(jnp.int32)
        back_z = lax.rem(rest, deep)
        return back_y, rest // deep, back_z

    row_path = path(offset_ref[0])
    column_path = path(offset_ref[0] - 1)

    def slot_x(whole):
        _, back_x, back_z = whole
        return lax.rem(back_x + (at_z + back_z >= deep).astype(jnp.int32), across)

    nothing = jnp.zeros((5, around, radial), jnp.float32)

    def clear(k, carry):
        field[k, :, 0] = nothing
        field[k, :, layers + 1] = nothing

        @pl.when(jnp.logical_not(has_below))
        def _():
            from_below[k] = nothing

        @pl.when(jnp.logical_not(has_above))
        def _():
            from_above[k] = nothing

        @pl.when(is_facing)
        def _():
            message_x[k, 5] = jnp.zeros((around, radial), jnp.float32)

        return carry

    lax.fori_loop(0, ITERS, clear, 0)

    def masks(count):
        shape = (count, around, radial)
        rows = lax.broadcasted_iota(jnp.int32, shape, 1)
        lanes = lax.broadcasted_iota(jnp.int32, shape, 2)
        return rows == 0, rows == around - 1, lanes == 0, lanes == radial - 1

    def pack(k, some, value):
        first_columns[k, :, some] = value[:, :, 0:1]
        last_columns[k, :, some] = value[:, :, around - 1 : around]

    def send(k):
        to_left(k).start()
        to_right(k).start()

        @pl.when(has_below)
        def _():
            downward(k).start()

        @pl.when(jnp.logical_and(has_above, jnp.logical_not(is_facing)))
        def _():
            upward(k).start()

        @pl.when(is_facing)
        def _():
            for distance in sorted(range(1, along), key=lambda d: -min(d, along - d)):
                row_y(k, distance).start()
            slots_y[k, 0] = field[k, :, layers]

    def pick(index, choices):
        value = choices[0]
        wanted = jnp.broadcast_to(index, value.shape)
        for place_back in range(1, len(choices)):
            value = jnp.where(wanted == place_back, choices[place_back], value)
        return value

    def turn_x(k):
        for distance in range(1, along):
            row_y(k, distance).wait_recv()
        message_x[k, pl.ds(0, 5)] = pick(row_path[0], [slots_y[k, back] for back in range(along)])
        message_x[k, 5, pl.ds(0, 5)] = pick(
            column_path[0], [slots_y[k, back, :, 0] for back in range(along)]
        )
        for distance in sorted(range(1, across), key=lambda d: -min(d, across - d)):
            row_x(k, distance).start()
        slots_x[k, 0] = message_x[k]

    def turn_z(k):
        for distance in range(1, across):
            row_x(k, distance).wait_recv()
        message_z[k, pl.ds(0, 5)] = pick(
            slot_x(row_path), [slots_x[k, back, pl.ds(0, 5)] for back in range(across)]
        )
        message_z[k, 5] = pick(slot_x(column_path), [slots_x[k, back, 5] for back in range(across)])
        for distance in range(deep):
            row_z(k, distance).start()

    def receive_axial(k):
        @pl.when(has_above)
        def _():
            downward(k).wait_recv()

        @pl.when(jnp.logical_and(has_below, jnp.logical_not(is_faced)))
        def _():
            upward(k).wait_recv()

        @pl.when(is_faced)
        def _():
            for distance in range(deep):
                row_z(k, distance).wait_recv()
            blend_facing(k)

    def blend_facing(k):
        rows = lax.broadcasted_iota(jnp.int32, (around, radial), 0)
        donors = jnp.zeros((around, radial), jnp.int32)
        shares = jnp.zeros((around, radial), jnp.float32)
        for cell in range(around):
            donors = jnp.where(rows == cell, cells_ref[cell], donors)
            shares = jnp.where(rows == cell, weights_ref[cell], shares)
        facing = pick(row_path[2], [slots_z[k, back, pl.ds(0, 5)] for back in range(deep)])
        extra = pick(column_path[2], [slots_z[k, back, 5] for back in range(deep)])
        blended = nothing
        for column in range(around + 1):
            share = jnp.where(donors == column, shares, jnp.where(donors == column - 1, 1.0 - shares, 0.0))
            if column < around:
                row = facing[:, column : column + 1]
            else:
                row = jnp.stack([extra[comp : comp + 1] for comp in range(5)])
            blended = blended + share[None] * jnp.broadcast_to(row, (5, around, radial))
        from_below[k] = blended

    def begin(k, low, count):
        some = pl.ds(low, count)
        top, bottom, hub, shroud = masks(count)
        total = source[:, some]
        for comp in range(5):
            here = field[k, comp, pl.ds(low + 1, count)]
            mixed = (
                0.6 * field[k, comp, some] + 0.4 * field[k, comp, pl.ds(low + 2, count)],
                0.6 * jnp.where(top, 0.0, pltpu.roll(here, 1, 1))
                + 0.4 * jnp.where(bottom, 0.0, pltpu.roll(here, around - 1, 1)),
                0.6 * jnp.where(hub, 0.0, pltpu.roll(here, 1, 2))
                + 0.4 * jnp.where(shroud, 0.0, pltpu.roll(here, radial - 1, 2)),
            )
            for direction in range(3):
                total = total + faces[direction, comp, :, some] * mixed[direction][None]
        partial[:, some] = total

    def add_axial(k, layer, share, halo):
        total = partial[:, layer]
        for comp in range(5):
            total = total + faces[0, comp, :, layer] * (share * halo[k, comp])[None]
        partial[:, layer] = total

    def finish(k, low, count):
        some = pl.ds(low, count)
        top, bottom, _, _ = masks(count)
        total = partial[:, some]
        for comp in range(5):
            behind = jnp.broadcast_to(0.6 * from_left[k, comp, some], (count, around, radial))
            ahead = jnp.broadcast_to(0.4 * from_right[k, comp, some], (count, around, radial))
            mixed = jnp.where(top, behind, jnp.where(bottom, ahead, 0.0))
            total = total + faces[1, comp, :, some] * mixed[None]
        value = inverse[0, :, some] * total[0][None]
        for comp in range(1, 5):
            value = value + inverse[comp, :, some] * total[comp][None]
        field[k + 1, :, pl.ds(low + 1, count)] = value
        pack(k + 1, some, value)

    load_prev.wait()
    pack(0, pl.ds(0, layers), field[0, :, pl.ds(1, layers)])

    ends = jnp.logical_or(block == 0, block == blocks - 1)
    ends_extra = 0 if blocks > 2 else -1

    @pl.when(is_facing)
    def _():
        pl.semaphore_wait(barrier, 3 + ends_extra + (along - 1) + (across - 1) + deep)

    @pl.when(jnp.logical_and(ends, jnp.logical_not(is_facing)))
    def _():
        pl.semaphore_wait(barrier, 3)

    @pl.when(jnp.logical_not(jnp.logical_or(ends, is_facing)))
    def _():
        pl.semaphore_wait(barrier, 4)

    half = layers // 2
    inner = half - 1

    def widen_faces(index, carry):
        direction, comp = index // 5, lax.rem(index, 5)
        faces[direction, comp] = faces_narrow[direction, comp].astype(jnp.float32)
        return carry

    def widen_inverse(index, carry):
        onto, comp = index // 5, lax.rem(index, 5)
        inverse[comp, onto] = inverse_narrow[onto, comp].astype(jnp.float32)
        return carry

    def sweep(k, carry):
        send(k)

        @pl.when(k == 0)
        def _():
            load_faces.wait()
            load_inverse.wait()
            lax.fori_loop(0, 15, widen_faces, 0)
            lax.fori_loop(0, 25, widen_inverse, 0)
            load_source.wait()

        @pl.when(jnp.logical_and(is_facing, lax.rem(k, 2) == 1))
        def _():
            for earlier in (1, 0):
                turn_x(k - earlier)
                turn_z(k - earlier)

        begin(k, 0, half)
        begin(k, half, half)
        to_left(k).wait_recv()
        to_right(k).wait_recv()
        finish(k, 1, inner)
        finish(k, half, inner)
        receive_axial(k)
        add_axial(k, 0, 0.6, from_below)
        add_axial(k, layers - 1, 0.4, from_above)
        finish(k, 0, 1)
        finish(k, layers - 1, 1)
        return carry

    lax.fori_loop(0, ITERS, sweep, 0)
    result = field[ITERS, :, pl.ds(1, layers)]
    out_ref[...] = result
    update_ref[...] = result - field[ITERS - 1, :, pl.ds(1, layers)]

    def settle(k, carry):
        to_left(k).wait_send()
        to_right(k).wait_send()

        @pl.when(has_below)
        def _():
            downward(k).wait_send()

        @pl.when(jnp.logical_and(has_above, jnp.logical_not(is_facing)))
        def _():
            upward(k).wait_send()

        @pl.when(is_facing)
        def _():
            for distance in range(1, along):
                row_y(k, distance).wait_send()
            for distance in range(1, across):
                row_x(k, distance).wait_send()
            for distance in range(deep):
                row_z(k, distance).wait_send()

        return carry

    lax.fori_loop(0, ITERS, settle, 0)


def swept(sectors, blocks, *args):
    layers, around, radial = args[0].shape[1:]
    across, deep, along = radices(sectors)
    f32 = jnp.float32
    cells = (5, layers, around, radial)
    anywhere = pl.BlockSpec(memory_space=pl.ANY)
    scalars = pl.BlockSpec(memory_space=pltpu.SMEM)
    vmem = pl.BlockSpec(memory_space=pltpu.VMEM)
    dma = pltpu.SemaphoreType.DMA
    return pl.pallas_call(
        functools.partial(kernel, sectors, blocks),
        out_shape=[OUT(cells, f32)] * 2,
        in_specs=[anywhere] * 4 + [scalars] * 3,
        out_specs=[vmem] * 2,
        scratch_shapes=[
            pltpu.VMEM((ITERS + 1, 5, layers + 2, around, radial), f32),
            pltpu.VMEM(cells, f32),
            pltpu.VMEM(cells, f32),
            pltpu.VMEM((3, 5, 5, layers, around, radial), jnp.bfloat16),
            pltpu.VMEM((5, 5, layers, around, radial), jnp.bfloat16),
            pltpu.VMEM((3, 5, 5, layers, around, radial), f32),
            pltpu.VMEM((5, 5, layers, around, radial), f32),
            pltpu.VMEM((ITERS + 1, 5, layers, 1, radial), f32),
            pltpu.VMEM((ITERS + 1, 5, layers, 1, radial), f32),
            pltpu.VMEM((ITERS, 5, layers, 1, radial), f32),
            pltpu.VMEM((ITERS, 5, layers, 1, radial), f32),
            pltpu.VMEM((ITERS, 5, around, radial), f32),
            pltpu.VMEM((ITERS, 5, around, radial), f32),
            pltpu.VMEM((ITERS, along, 5, around, radial), f32),
            pltpu.VMEM((ITERS, 6, around, radial), f32),
            pltpu.VMEM((ITERS, across, 6, around, radial), f32),
            pltpu.VMEM((ITERS, 6, around, radial), f32),
            pltpu.VMEM((ITERS, deep, 6, around, radial), f32),
            dma((4,)),
            dma((ITERS, 4)),
            dma((ITERS, 4)),
            dma((ITERS, along)),
            dma((ITERS, along)),
            dma((ITERS, across)),
            dma((ITERS, across)),
            dma((ITERS, deep)),
            dma((ITERS, deep)),
        ],
        compiler_params=pltpu.CompilerParams(collective_id=0, has_side_effects=True),
        name="sweeps",
    )(*args)


OUT = pltpu.VMEM


def put_kernel(first_ref, second_ref, first_out, second_out, sems):
    copies = (
        pltpu.make_async_copy(first_ref, first_out, sems.at[0]),
        pltpu.make_async_copy(second_ref, second_out, sems.at[1]),
    )
    for copy in copies:
        copy.start()
    for copy in copies:
        copy.wait()


def put(*values):
    anywhere = pl.BlockSpec(memory_space=pl.ANY)
    return pl.pallas_call(
        put_kernel,
        out_shape=[jax.ShapeDtypeStruct(value.shape, value.dtype) for value in values],
        in_specs=[anywhere] * 2,
        out_specs=[anywhere] * 2,
        scratch_shapes=[pltpu.SemaphoreType.DMA((2,))],
        name="put",
    )(*values)


def shards(prev, source, faces, inverse, sector_offset, donor_cells, donor_weights):
    result = swept(
        lax.axis_size("sector"),
        lax.axis_size("block"),
        prev,
        source,
        faces,
        inverse,
        sector_offset,
        donor_cells,
        donor_weights,
    )
    return tuple(result)


def solution(mesh):
    return jax.shard_map(
        shards,
        mesh=mesh,
        in_specs=(
            P(None, "block", "sector", None),
            P(None, "block", "sector", None),
            P(None, None, None, "block", "sector", None),
            P(None, None, "block", "sector", None),
            P(),
            P("sector"),
            P("sector"),
        ),
        out_specs=(P(None, "block", "sector", None), P(None, "block", "sector", None)),
        check_vma=False,
    )
```

```python
import functools

import jax
import jax.numpy as jnp
from jax import lax
from jax.experimental import pallas as pl
from jax.experimental.pallas import tpu as pltpu
from jax.sharding import PartitionSpec as P

ITERS = 4
MESH = pl.DeviceIdType.MESH
LEFT, RIGHT, DOWN, UP = range(4)


def radices(sectors):
    return (sectors // 16, 2, 8) if sectors >= 16 else (2, 2, 2)


def kernel(
    turn,
    sectors,
    blocks,
    prev_ref,
    source_ref,
    faces_ref,
    inverse_ref,
    offset_ref,
    cells_ref,
    weights_ref,
    out_ref,
    update_ref,
    field,
    partial,
    source,
    faces_narrow,
    inverse_narrow,
    faces,
    inverse,
    first_columns,
    last_columns,
    from_left,
    from_right,
    from_below,
    from_above,
    slots_y,
    slots_c,
    message_x,
    slots_x,
    message_z,
    slots_z,
    load_sems,
    send_sems,
    recv_sems,
    send_y,
    recv_y,
    send_x,
    recv_x,
    send_z,
    recv_z,
):
    layers, around, radial = prev_ref.shape[1:]
    across, deep, along = radices(sectors)
    group = deep * along
    column_turn = (turn - 1) % along
    sector = lax.axis_index("sector")
    block = lax.axis_index("block")
    at_x = sector // group
    at_z = lax.rem(sector // along, deep)
    at_y = lax.rem(sector, along)
    left = lax.rem(sector + sectors - 1, sectors)
    right = lax.rem(sector + 1, sectors)
    is_facing = block == blocks // 2 - 1
    is_faced = block == blocks // 2
    has_above = block < blocks - 1
    has_below = block > 0

    def place(x, z, y):
        return x * group + z * along + y

    def moved_y(distance):
        return place(at_x, at_z, lax.rem(at_y + distance + along, along))

    def moved_x(distance):
        return place(lax.rem(at_x + distance + across, across), at_z, at_y)

    def moved_z(distance):
        return place(at_x, lax.rem(at_z + distance + deep, deep), at_y)

    barrier = pltpu.get_barrier_semaphore()

    def greet(to_sector, to_block):
        pl.semaphore_signal(barrier, inc=1, device_id=(to_sector, to_block), device_id_type=MESH)

    @pl.when(is_faced)
    def _():
        for distance in range(deep):
            greet(moved_z(-distance), block - 1)

    @pl.when(is_facing)
    def _():
        for distance in (turn, column_turn):
            if distance:
                greet(moved_y(-distance), block)
        for distance in range(1, across):
            greet(moved_x(-distance), block)

    greet(left, block)
    greet(right, block)

    @pl.when(has_above)
    def _():
        greet(sector, block + 1)

    @pl.when(jnp.logical_and(has_below, jnp.logical_not(is_faced)))
    def _():
        greet(sector, block - 1)

    def load(index, src, dst):
        return pltpu.make_async_copy(src, dst, load_sems.at[index])

    load_prev = load(0, prev_ref, field.at[0, :, pl.ds(1, layers)])
    load_source = load(1, source_ref, source)
    load_faces = load(2, faces_ref, faces_narrow)
    load_inverse = load(3, inverse_ref, inverse_narrow)
    load_prev.start()
    load_faces.start()
    load_inverse.start()
    load_source.start()

    def remote(src, dst, send_sem, recv_sem, to_sector, to_block):
        return pltpu.make_async_remote_copy(
            src_ref=src,
            dst_ref=dst,
            send_sem=send_sem,
            recv_sem=recv_sem,
            device_id=(to_sector, to_block),
            device_id_type=MESH,
        )

    def step_copy(k, direction, src, dst, to_sector, to_block):
        return remote(src, dst, send_sems.at[k, direction], recv_sems.at[k, direction], to_sector, to_block)

    def to_left(k):
        return step_copy(k, LEFT, first_columns.at[k], from_right.at[k], left, block)

    def to_right(k):
        return step_copy(k, RIGHT, last_columns.at[k], from_left.at[k], right, block)

    def downward(k):
        return step_copy(k, DOWN, field.at[k, :, 1], from_above.at[k], sector, block - 1)

    def upward(k):
        return step_copy(k, UP, field.at[k, :, layers], from_below.at[k], sector, block + 1)

    def row_y(k):
        return remote(
            field.at[k, :, layers], slots_y.at[k], send_y.at[k, 0], recv_y.at[k, 0], moved_y(turn), block
        )

    def column_y(k):
        return remote(
            first_columns.at[k, :, layers - 1],
            slots_c.at[k],
            send_y.at[k, 1],
            recv_y.at[k, 1],
            moved_y(column_turn),
            block,
        )

    def row_x(k, distance):
        return remote(
            message_x.at[k],
            slots_x.at[k, distance],
            send_x.at[k, distance],
            recv_x.at[k, distance],
            moved_x(distance),
            block,
        )

    def row_z(k, distance):
        return remote(
            message_z.at[k],
            slots_z.at[k, distance],
            send_z.at[k, distance],
            recv_z.at[k, distance],
            moved_z(distance),
            block + 1,
        )

    def path(offset):
        back_y = lax.rem(offset, along)
        rest = offset // along + (at_y < back_y).astype(jnp.int32)
        back_z = lax.rem(rest, deep)
        return back_y, rest // deep, back_z

    row_path = path(offset_ref[0])
    column_path = path(offset_ref[0] - 1)

    def slot_x(whole):
        _, back_x, back_z = whole
        return lax.rem(back_x + (at_z + back_z >= deep).astype(jnp.int32), across)

    nothing = jnp.zeros((5, around, radial), jnp.float32)

    def clear(k, carry):
        field[k, :, 0] = nothing
        field[k, :, layers + 1] = nothing

        @pl.when(jnp.logical_not(has_below))
        def _():
            from_below[k] = nothing

        @pl.when(jnp.logical_not(has_above))
        def _():
            from_above[k] = nothing

        @pl.when(is_facing)
        def _():
            message_x[k, 5] = jnp.zeros((around, radial), jnp.float32)

        return carry

    lax.fori_loop(0, ITERS, clear, 0)

    def masks(count):
        shape = (count, around, radial)
        rows = lax.broadcasted_iota(jnp.int32, shape, 1)
        lanes = lax.broadcasted_iota(jnp.int32, shape, 2)
        return rows == 0, rows == around - 1, lanes == 0, lanes == radial - 1

    def pack(k, some, value):
        first_columns[k, :, some] = value[:, :, 0:1]
        last_columns[k, :, some] = value[:, :, around - 1 : around]

    def send(k):
        to_left(k).start()
        to_right(k).start()

        @pl.when(has_below)
        def _():
            downward(k).start()

        @pl.when(jnp.logical_and(has_above, jnp.logical_not(is_facing)))
        def _():
            upward(k).start()

        @pl.when(is_facing)
        def _():
            if turn:
                row_y(k).start()
            if column_turn:
                column_y(k).start()

    def pick(index, choices):
        value = choices[0]
        wanted = jnp.broadcast_to(index, value.shape)
        for place_back in range(1, len(choices)):
            value = jnp.where(wanted == place_back, choices[place_back], value)
        return value

    def turn_x(k):
        if turn:
            row_y(k).wait_recv()
            message_x[k, pl.ds(0, 5)] = slots_y[k]
        else:
            message_x[k, pl.ds(0, 5)] = field[k, :, layers]
        if column_turn:
            column_y(k).wait_recv()
            message_x[k, 5, pl.ds(0, 5)] = slots_c[k, :, 0]
        else:
            message_x[k, 5, pl.ds(0, 5)] = field[k, :, layers, 0]
        for distance in sorted(range(1, across), key=lambda d: -min(d, across - d)):
            row_x(k, distance).start()
        slots_x[k, 0] = message_x[k]

    def turn_z(k):
        for distance in range(1, across):
            row_x(k, distance).wait_recv()
        message_z[k, pl.ds(0, 5)] = pick(
            slot_x(row_path), [slots_x[k, back, pl.ds(0, 5)] for back in range(across)]
        )
        message_z[k, 5] = pick(slot_x(column_path), [slots_x[k, back, 5] for back in range(across)])
        for distance in range(deep):
            row_z(k, distance).start()

    def receive_axial(k):
        @pl.when(has_above)
        def _():
            downward(k).wait_recv()

        @pl.when(jnp.logical_and(has_below, jnp.logical_not(is_faced)))
        def _():
            upward(k).wait_recv()

        @pl.when(is_faced)
        def _():
            for distance in range(deep):
                row_z(k, distance).wait_recv()
            blend_facing(k)

    def blend_facing(k):
        rows = lax.broadcasted_iota(jnp.int32, (around, radial), 0)
        donors = jnp.zeros((around, radial), jnp.int32)
        shares = jnp.zeros((around, radial), jnp.float32)
        for cell in range(around):
            donors = jnp.where(rows == cell, cells_ref[cell], donors)
            shares = jnp.where(rows == cell, weights_ref[cell], shares)
        facing = pick(row_path[2], [slots_z[k, back, pl.ds(0, 5)] for back in range(deep)])
        extra = pick(column_path[2], [slots_z[k, back, 5] for back in range(deep)])
        blended = nothing
        for column in range(around + 1):
            share = jnp.where(donors == column, shares, jnp.where(donors == column - 1, 1.0 - shares, 0.0))
            if column < around:
                row = facing[:, column : column + 1]
            else:
                row = jnp.stack([extra[comp : comp + 1] for comp in range(5)])
            blended = blended + share[None] * jnp.broadcast_to(row, (5, around, radial))
        from_below[k] = blended

    def begin(k, low, count):
        some = pl.ds(low, count)
        top, bottom, hub, shroud = masks(count)
        total = source[:, some]
        for comp in range(5):
            here = field[k, comp, pl.ds(low + 1, count)]
            mixed = (
                0.6 * field[k, comp, some] + 0.4 * field[k, comp, pl.ds(low + 2, count)],
                0.6 * jnp.where(top, 0.0, pltpu.roll(here, 1, 1))
                + 0.4 * jnp.where(bottom, 0.0, pltpu.roll(here, around - 1, 1)),
                0.6 * jnp.where(hub, 0.0, pltpu.roll(here, 1, 2))
                + 0.4 * jnp.where(shroud, 0.0, pltpu.roll(here, radial - 1, 2)),
            )
            for direction in range(3):
                total = total + faces[direction, comp, :, some] * mixed[direction][None]
        partial[:, some] = total

    def add_axial(k, layer, share, halo):
        total = partial[:, layer]
        for comp in range(5):
            total = total + faces[0, comp, :, layer] * (share * halo[k, comp])[None]
        partial[:, layer] = total

    def finish(k, low, count):
        some = pl.ds(low, count)
        top, bottom, _, _ = masks(count)
        total = partial[:, some]
        for comp in range(5):
            behind = jnp.broadcast_to(0.6 * from_left[k, comp, some], (count, around, radial))
            ahead = jnp.broadcast_to(0.4 * from_right[k, comp, some], (count, around, radial))
            mixed = jnp.where(top, behind, jnp.where(bottom, ahead, 0.0))
            total = total + faces[1, comp, :, some] * mixed[None]
        value = inverse[0, :, some] * total[0][None]
        for comp in range(1, 5):
            value = value + inverse[comp, :, some] * total[comp][None]
        field[k + 1, :, pl.ds(low + 1, count)] = value
        pack(k + 1, some, value)

    load_prev.wait()
    pack(0, pl.ds(0, layers), field[0, :, pl.ds(1, layers)])

    ends = jnp.logical_or(block == 0, block == blocks - 1)
    ends_extra = 0 if blocks > 2 else -1

    @pl.when(is_facing)
    def _():
        pl.semaphore_wait(barrier, 3 + ends_extra + bool(turn) + bool(column_turn) + (across - 1) + deep)

    @pl.when(jnp.logical_and(ends, jnp.logical_not(is_facing)))
    def _():
        pl.semaphore_wait(barrier, 3)

    @pl.when(jnp.logical_not(jnp.logical_or(ends, is_facing)))
    def _():
        pl.semaphore_wait(barrier, 4)

    half = layers // 2
    inner = half - 1

    def widen_faces(index, carry):
        direction, comp = index // 5, lax.rem(index, 5)
        faces[direction, comp] = faces_narrow[direction, comp].astype(jnp.float32)
        return carry

    def widen_inverse(index, carry):
        onto, comp = index // 5, lax.rem(index, 5)
        inverse[comp, onto] = inverse_narrow[onto, comp].astype(jnp.float32)
        return carry

    def sweep(k, carry):
        send(k)

        @pl.when(k == 0)
        def _():
            load_faces.wait()
            load_inverse.wait()
            lax.fori_loop(0, 15, widen_faces, 0)
            lax.fori_loop(0, 25, widen_inverse, 0)
            load_source.wait()

        @pl.when(jnp.logical_and(is_facing, lax.rem(k, 2) == 1))
        def _():
            for earlier in (1, 0):
                turn_x(k - earlier)
                turn_z(k - earlier)

        begin(k, 0, half)
        begin(k, half, half)
        to_left(k).wait_recv()
        to_right(k).wait_recv()
        finish(k, 1, inner)
        finish(k, half, inner)
        receive_axial(k)
        add_axial(k, 0, 0.6, from_below)
        add_axial(k, layers - 1, 0.4, from_above)
        finish(k, 0, 1)
        finish(k, layers - 1, 1)
        return carry

    lax.fori_loop(0, ITERS, sweep, 0)
    result = field[ITERS, :, pl.ds(1, layers)]
    out_ref[...] = result
    update_ref[...] = result - field[ITERS - 1, :, pl.ds(1, layers)]

    def settle(k, carry):
        to_left(k).wait_send()
        to_right(k).wait_send()

        @pl.when(has_below)
        def _():
            downward(k).wait_send()

        @pl.when(jnp.logical_and(has_above, jnp.logical_not(is_facing)))
        def _():
            upward(k).wait_send()

        @pl.when(is_facing)
        def _():
            if turn:
                row_y(k).wait_send()
            if column_turn:
                column_y(k).wait_send()
            for distance in range(1, across):
                row_x(k, distance).wait_send()
            for distance in range(deep):
                row_z(k, distance).wait_send()

        return carry

    lax.fori_loop(0, ITERS, settle, 0)


def swept(turn, sectors, blocks, *args):
    layers, around, radial = args[0].shape[1:]
    across, deep, along = radices(sectors)
    f32 = jnp.float32
    cells = (5, layers, around, radial)
    anywhere = pl.BlockSpec(memory_space=pl.ANY)
    scalars = pl.BlockSpec(memory_space=pltpu.SMEM)
    vmem = pl.BlockSpec(memory_space=pltpu.VMEM)
    dma = pltpu.SemaphoreType.DMA
    return pl.pallas_call(
        functools.partial(kernel, turn, sectors, blocks),
        out_shape=[OUT(cells, f32)] * 2,
        in_specs=[anywhere] * 4 + [scalars] * 3,
        out_specs=[vmem] * 2,
        scratch_shapes=[
            pltpu.VMEM((ITERS + 1, 5, layers + 2, around, radial), f32),
            pltpu.VMEM(cells, f32),
            pltpu.VMEM(cells, f32),
            pltpu.VMEM((3, 5, 5, layers, around, radial), jnp.bfloat16),
            pltpu.VMEM((5, 5, layers, around, radial), jnp.bfloat16),
            pltpu.VMEM((3, 5, 5, layers, around, radial), f32),
            pltpu.VMEM((5, 5, layers, around, radial), f32),
            pltpu.VMEM((ITERS + 1, 5, layers, 1, radial), f32),
            pltpu.VMEM((ITERS + 1, 5, layers, 1, radial), f32),
            pltpu.VMEM((ITERS, 5, layers, 1, radial), f32),
            pltpu.VMEM((ITERS, 5, layers, 1, radial), f32),
            pltpu.VMEM((ITERS, 5, around, radial), f32),
            pltpu.VMEM((ITERS, 5, around, radial), f32),
            pltpu.VMEM((ITERS, 5, around, radial), f32),
            pltpu.VMEM((ITERS, 5, 1, radial), f32),
            pltpu.VMEM((ITERS, 6, around, radial), f32),
            pltpu.VMEM((ITERS, across, 6, around, radial), f32),
            pltpu.VMEM((ITERS, 6, around, radial), f32),
            pltpu.VMEM((ITERS, deep, 6, around, radial), f32),
            dma((4,)),
            dma((ITERS, 4)),
            dma((ITERS, 4)),
            dma((ITERS, 2)),
            dma((ITERS, 2)),
            dma((ITERS, across)),
            dma((ITERS, across)),
            dma((ITERS, deep)),
            dma((ITERS, deep)),
        ],
        compiler_params=pltpu.CompilerParams(collective_id=turn, has_side_effects=True),
        name="sweeps",
    )(*args)


OUT = pltpu.VMEM


def put_kernel(first_ref, second_ref, first_out, second_out, sems):
    copies = (
        pltpu.make_async_copy(first_ref, first_out, sems.at[0]),
        pltpu.make_async_copy(second_ref, second_out, sems.at[1]),
    )
    for copy in copies:
        copy.start()
    for copy in copies:
        copy.wait()


def put(*values):
    anywhere = pl.BlockSpec(memory_space=pl.ANY)
    return pl.pallas_call(
        put_kernel,
        out_shape=[jax.ShapeDtypeStruct(value.shape, value.dtype) for value in values],
        in_specs=[anywhere] * 2,
        out_specs=[anywhere] * 2,
        scratch_shapes=[pltpu.SemaphoreType.DMA((2,))],
        name="put",
    )(*values)


def shards(prev, source, faces, inverse, sector_offset, donor_cells, donor_weights):
    sectors = lax.axis_size("sector")
    along = radices(sectors)[2]
    branches = [functools.partial(swept, turn, sectors, lax.axis_size("block")) for turn in range(along)]
    result = lax.switch(
        lax.rem(sector_offset[0], along),
        branches,
        prev,
        source,
        faces,
        inverse,
        sector_offset,
        donor_cells,
        donor_weights,
    )
    return tuple(result)


def solution(mesh):
    return jax.shard_map(
        shards,
        mesh=mesh,
        in_specs=(
            P(None, "block", "sector", None),
            P(None, "block", "sector", None),
            P(None, None, None, "block", "sector", None),
            P(None, None, "block", "sector", None),
            P(),
            P("sector"),
            P("sector"),
        ),
        out_specs=(P(None, "block", "sector", None), P(None, "block", "sector", None)),
        check_vma=False,
    )
```

```python
import functools

import jax
import jax.numpy as jnp
from jax import lax
from jax.experimental import pallas as pl
from jax.experimental.pallas import tpu as pltpu
from jax.sharding import PartitionSpec as P

ITERS = 4
MESH = pl.DeviceIdType.MESH
LEFT, RIGHT, DOWN, UP = range(4)


def radices(sectors):
    return (sectors // 16, 2, 8) if sectors >= 16 else (2, 2, 2)


def kernel(
    turn,
    sectors,
    blocks,
    prev_ref,
    source_ref,
    faces_ref,
    inverse_ref,
    offset_ref,
    cells_ref,
    weights_ref,
    out_ref,
    update_ref,
    field,
    partial,
    source,
    faces_narrow,
    inverse_narrow,
    faces,
    inverse,
    first_columns,
    last_columns,
    from_left,
    from_right,
    from_below,
    from_above,
    slots_y,
    slots_c,
    message_x,
    slots_x,
    message_z,
    slots_z,
    load_sems,
    send_sems,
    recv_sems,
    send_y,
    recv_y,
    send_x,
    recv_x,
    send_z,
    recv_z,
):
    layers, around, radial = prev_ref.shape[1:]
    across, deep, along = radices(sectors)
    group = deep * along
    column_turn = (turn - 1) % along
    sector = lax.axis_index("sector")
    block = lax.axis_index("block")
    at_x = sector // group
    at_z = lax.rem(sector // along, deep)
    at_y = lax.rem(sector, along)
    left = lax.rem(sector + sectors - 1, sectors)
    right = lax.rem(sector + 1, sectors)
    is_facing = block == blocks // 2 - 1
    is_faced = block == blocks // 2
    has_above = block < blocks - 1
    has_below = block > 0

    def place(x, z, y):
        return x * group + z * along + y

    def moved_y(distance):
        return place(at_x, at_z, lax.rem(at_y + distance + along, along))

    def moved_x(distance):
        return place(lax.rem(at_x + distance + across, across), at_z, at_y)

    def moved_z(distance):
        return place(at_x, lax.rem(at_z + distance + deep, deep), at_y)

    barrier = pltpu.get_barrier_semaphore()

    def greet(to_sector, to_block):
        pl.semaphore_signal(barrier, inc=1, device_id=(to_sector, to_block), device_id_type=MESH)

    @pl.when(is_faced)
    def _():
        for distance in range(deep):
            greet(moved_z(-distance), block - 1)

    @pl.when(is_facing)
    def _():
        for distance in (turn, column_turn):
            if distance:
                greet(moved_y(-distance), block)
        for distance in range(1, across):
            greet(moved_x(-distance), block)

    greet(left, block)
    greet(right, block)

    @pl.when(has_above)
    def _():
        greet(sector, block + 1)

    @pl.when(jnp.logical_and(has_below, jnp.logical_not(is_faced)))
    def _():
        greet(sector, block - 1)

    def load(index, src, dst):
        return pltpu.make_async_copy(src, dst, load_sems.at[index])

    load_prev = load(0, prev_ref, field.at[0, :, pl.ds(1, layers)])
    load_source = load(1, source_ref, source)
    load_faces = load(2, faces_ref, faces_narrow)
    load_inverse = load(3, inverse_ref, inverse_narrow)
    load_prev.start()
    load_faces.start()
    load_inverse.start()
    load_source.start()

    def remote(src, dst, send_sem, recv_sem, to_sector, to_block):
        return pltpu.make_async_remote_copy(
            src_ref=src,
            dst_ref=dst,
            send_sem=send_sem,
            recv_sem=recv_sem,
            device_id=(to_sector, to_block),
            device_id_type=MESH,
        )

    def step_copy(k, direction, src, dst, to_sector, to_block):
        return remote(src, dst, send_sems.at[k, direction], recv_sems.at[k, direction], to_sector, to_block)

    def to_left(k):
        return step_copy(k, LEFT, first_columns.at[k], from_right.at[k], left, block)

    def to_right(k):
        return step_copy(k, RIGHT, last_columns.at[k], from_left.at[k], right, block)

    def downward(k):
        return step_copy(k, DOWN, field.at[k, :, 1], from_above.at[k], sector, block - 1)

    def upward(k):
        return step_copy(k, UP, field.at[k, :, layers], from_below.at[k], sector, block + 1)

    def row_y(k):
        return remote(
            field.at[k, :, layers], slots_y.at[k], send_y.at[k, 0], recv_y.at[k, 0], moved_y(turn), block
        )

    def column_y(k):
        return remote(
            first_columns.at[k, :, layers - 1],
            slots_c.at[k],
            send_y.at[k, 1],
            recv_y.at[k, 1],
            moved_y(column_turn),
            block,
        )

    def row_x(k, distance):
        return remote(
            message_x.at[k],
            slots_x.at[k, distance],
            send_x.at[k, distance],
            recv_x.at[k, distance],
            moved_x(distance),
            block,
        )

    def row_z(k, distance):
        return remote(
            message_z.at[k],
            slots_z.at[k, distance],
            send_z.at[k, distance],
            recv_z.at[k, distance],
            moved_z(distance),
            block + 1,
        )

    def path(offset):
        back_y = lax.rem(offset, along)
        rest = offset // along + (at_y < back_y).astype(jnp.int32)
        back_z = lax.rem(rest, deep)
        return back_y, rest // deep, back_z

    row_path = path(offset_ref[0])
    column_path = path(offset_ref[0] - 1)

    def slot_x(whole):
        _, back_x, back_z = whole
        return lax.rem(back_x + (at_z + back_z >= deep).astype(jnp.int32), across)

    nothing = jnp.zeros((5, around, radial), jnp.float32)

    def clear(k, carry):
        field[k, :, 0] = nothing
        field[k, :, layers + 1] = nothing

        @pl.when(jnp.logical_not(has_below))
        def _():
            from_below[k] = nothing

        @pl.when(jnp.logical_not(has_above))
        def _():
            from_above[k] = nothing

        @pl.when(is_facing)
        def _():
            message_x[k, 5] = jnp.zeros((around, radial), jnp.float32)

        return carry

    lax.fori_loop(0, ITERS, clear, 0)

    def masks(count):
        shape = (count, around, radial)
        rows = lax.broadcasted_iota(jnp.int32, shape, 1)
        lanes = lax.broadcasted_iota(jnp.int32, shape, 2)
        return rows == 0, rows == around - 1, lanes == 0, lanes == radial - 1

    def pack(k, some, value):
        first_columns[k, :, some] = value[:, :, 0:1]
        last_columns[k, :, some] = value[:, :, around - 1 : around]

    def send(k):
        to_left(k).start()
        to_right(k).start()

        @pl.when(has_below)
        def _():
            downward(k).start()

        @pl.when(jnp.logical_and(has_above, jnp.logical_not(is_facing)))
        def _():
            upward(k).start()

        @pl.when(is_facing)
        def _():
            if turn:
                row_y(k).start()
            if column_turn:
                column_y(k).start()

    def pick(index, choices):
        value = choices[0]
        wanted = jnp.broadcast_to(index, value.shape)
        for place_back in range(1, len(choices)):
            value = jnp.where(wanted == place_back, choices[place_back], value)
        return value

    def turn_x(k):
        if turn:
            row_y(k).wait_recv()
            message_x[k, pl.ds(0, 5)] = slots_y[k]
        else:
            message_x[k, pl.ds(0, 5)] = field[k, :, layers]
        if column_turn:
            column_y(k).wait_recv()
            message_x[k, 5, pl.ds(0, 5)] = slots_c[k, :, 0]
        else:
            message_x[k, 5, pl.ds(0, 5)] = field[k, :, layers, 0]
        for distance in sorted(range(1, across), key=lambda d: -min(d, across - d)):
            row_x(k, distance).start()
        slots_x[k, 0] = message_x[k]

    def turn_z(k):
        for distance in range(1, across):
            row_x(k, distance).wait_recv()
        message_z[k, pl.ds(0, 5)] = pick(
            slot_x(row_path), [slots_x[k, back, pl.ds(0, 5)] for back in range(across)]
        )
        message_z[k, 5] = pick(slot_x(column_path), [slots_x[k, back, 5] for back in range(across)])
        for distance in range(deep):
            row_z(k, distance).start()

    def receive_axial(k):
        @pl.when(has_above)
        def _():
            downward(k).wait_recv()

        @pl.when(jnp.logical_and(has_below, jnp.logical_not(is_faced)))
        def _():
            upward(k).wait_recv()

        @pl.when(is_faced)
        def _():
            for distance in range(deep):
                row_z(k, distance).wait_recv()
            blend_facing(k)

    def blend_facing(k):
        rows = lax.broadcasted_iota(jnp.int32, (around, radial), 0)
        donors = jnp.zeros((around, radial), jnp.int32)
        shares = jnp.zeros((around, radial), jnp.float32)
        for cell in range(around):
            donors = jnp.where(rows == cell, cells_ref[cell], donors)
            shares = jnp.where(rows == cell, weights_ref[cell], shares)
        facing = pick(row_path[2], [slots_z[k, back, pl.ds(0, 5)] for back in range(deep)])
        extra = pick(column_path[2], [slots_z[k, back, 5] for back in range(deep)])
        blended = nothing
        for column in range(around + 1):
            share = jnp.where(donors == column, shares, jnp.where(donors == column - 1, 1.0 - shares, 0.0))
            if column < around:
                row = facing[:, column : column + 1]
            else:
                row = jnp.stack([extra[comp : comp + 1] for comp in range(5)])
            blended = blended + share[None] * jnp.broadcast_to(row, (5, around, radial))
        from_below[k] = blended

    def begin(k, low, count):
        some = pl.ds(low, count)
        top, bottom, hub, shroud = masks(count)
        total = source[:, some]
        for comp in range(5):
            here = field[k, comp, pl.ds(low + 1, count)]
            mixed = (
                0.6 * field[k, comp, some] + 0.4 * field[k, comp, pl.ds(low + 2, count)],
                0.6 * jnp.where(top, 0.0, pltpu.roll(here, 1, 1))
                + 0.4 * jnp.where(bottom, 0.0, pltpu.roll(here, around - 1, 1)),
                0.6 * jnp.where(hub, 0.0, pltpu.roll(here, 1, 2))
                + 0.4 * jnp.where(shroud, 0.0, pltpu.roll(here, radial - 1, 2)),
            )
            for direction in range(3):
                total = total + faces[direction, comp, :, some] * mixed[direction][None]
        partial[:, some] = total

    def add_axial(k, layer, share, halo):
        total = partial[:, layer]
        for comp in range(5):
            total = total + faces[0, comp, :, layer] * (share * halo[k, comp])[None]
        partial[:, layer] = total

    def finish(k, low, count):
        some = pl.ds(low, count)
        top, bottom, _, _ = masks(count)
        total = partial[:, some]
        for comp in range(5):
            behind = jnp.broadcast_to(0.6 * from_left[k, comp, some], (count, around, radial))
            ahead = jnp.broadcast_to(0.4 * from_right[k, comp, some], (count, around, radial))
            mixed = jnp.where(top, behind, jnp.where(bottom, ahead, 0.0))
            total = total + faces[1, comp, :, some] * mixed[None]
        value = inverse[0, :, some] * total[0][None]
        for comp in range(1, 5):
            value = value + inverse[comp, :, some] * total[comp][None]
        field[k + 1, :, pl.ds(low + 1, count)] = value
        pack(k + 1, some, value)

    load_prev.wait()
    pack(0, pl.ds(0, layers), field[0, :, pl.ds(1, layers)])

    ends = jnp.logical_or(block == 0, block == blocks - 1)
    ends_extra = 0 if blocks > 2 else -1

    @pl.when(is_facing)
    def _():
        pl.semaphore_wait(barrier, 3 + ends_extra + bool(turn) + bool(column_turn) + (across - 1) + deep)

    @pl.when(jnp.logical_and(ends, jnp.logical_not(is_facing)))
    def _():
        pl.semaphore_wait(barrier, 3)

    @pl.when(jnp.logical_not(jnp.logical_or(ends, is_facing)))
    def _():
        pl.semaphore_wait(barrier, 4)

    half = layers // 2
    inner = half - 1

    def widen_faces(index, carry):
        direction, comp = index // 5, lax.rem(index, 5)
        faces[direction, comp] = faces_narrow[direction, comp].astype(jnp.float32)
        return carry

    def widen_inverse(index, carry):
        onto, comp = index // 5, lax.rem(index, 5)
        inverse[comp, onto] = inverse_narrow[onto, comp].astype(jnp.float32)
        return carry

    def sweep(k, carry):
        send(k)

        @pl.when(k == 0)
        def _():
            load_faces.wait()
            load_inverse.wait()
            lax.fori_loop(0, 15, widen_faces, 0)
            lax.fori_loop(0, 25, widen_inverse, 0)
            load_source.wait()

        @pl.when(jnp.logical_and(is_facing, lax.rem(k, 2) == 1))
        def _():
            @pl.when(k > 1)
            def _():
                turn_x(k - 1)

            turn_z(k - 1)
            turn_x(k)
            turn_z(k)

        begin(k, 0, half)
        begin(k, half, half)

        @pl.when(jnp.logical_and(is_facing, k == 0))
        def _():
            turn_x(0)

        to_left(k).wait_recv()
        to_right(k).wait_recv()
        finish(k, 1, inner)
        finish(k, half, inner)
        receive_axial(k)
        add_axial(k, 0, 0.6, from_below)
        add_axial(k, layers - 1, 0.4, from_above)
        finish(k, 0, 1)
        finish(k, layers - 1, 1)
        return carry

    lax.fori_loop(0, ITERS, sweep, 0)
    result = field[ITERS, :, pl.ds(1, layers)]
    out_ref[...] = result
    update_ref[...] = result - field[ITERS - 1, :, pl.ds(1, layers)]

    def settle(k, carry):
        to_left(k).wait_send()
        to_right(k).wait_send()

        @pl.when(has_below)
        def _():
            downward(k).wait_send()

        @pl.when(jnp.logical_and(has_above, jnp.logical_not(is_facing)))
        def _():
            upward(k).wait_send()

        @pl.when(is_facing)
        def _():
            if turn:
                row_y(k).wait_send()
            if column_turn:
                column_y(k).wait_send()
            for distance in range(1, across):
                row_x(k, distance).wait_send()
            for distance in range(deep):
                row_z(k, distance).wait_send()

        return carry

    lax.fori_loop(0, ITERS, settle, 0)


def swept(turn, sectors, blocks, *args):
    layers, around, radial = args[0].shape[1:]
    across, deep, along = radices(sectors)
    f32 = jnp.float32
    cells = (5, layers, around, radial)
    anywhere = pl.BlockSpec(memory_space=pl.ANY)
    scalars = pl.BlockSpec(memory_space=pltpu.SMEM)
    vmem = pl.BlockSpec(memory_space=pltpu.VMEM)
    dma = pltpu.SemaphoreType.DMA
    return pl.pallas_call(
        functools.partial(kernel, turn, sectors, blocks),
        out_shape=[OUT(cells, f32)] * 2,
        in_specs=[anywhere] * 4 + [scalars] * 3,
        out_specs=[vmem] * 2,
        scratch_shapes=[
            pltpu.VMEM((ITERS + 1, 5, layers + 2, around, radial), f32),
            pltpu.VMEM(cells, f32),
            pltpu.VMEM(cells, f32),
            pltpu.VMEM((3, 5, 5, layers, around, radial), jnp.bfloat16),
            pltpu.VMEM((5, 5, layers, around, radial), jnp.bfloat16),
            pltpu.VMEM((3, 5, 5, layers, around, radial), f32),
            pltpu.VMEM((5, 5, layers, around, radial), f32),
            pltpu.VMEM((ITERS + 1, 5, layers, 1, radial), f32),
            pltpu.VMEM((ITERS + 1, 5, layers, 1, radial), f32),
            pltpu.VMEM((ITERS, 5, layers, 1, radial), f32),
            pltpu.VMEM((ITERS, 5, layers, 1, radial), f32),
            pltpu.VMEM((ITERS, 5, around, radial), f32),
            pltpu.VMEM((ITERS, 5, around, radial), f32),
            pltpu.VMEM((ITERS, 5, around, radial), f32),
            pltpu.VMEM((ITERS, 5, 1, radial), f32),
            pltpu.VMEM((ITERS, 6, around, radial), f32),
            pltpu.VMEM((ITERS, across, 6, around, radial), f32),
            pltpu.VMEM((ITERS, 6, around, radial), f32),
            pltpu.VMEM((ITERS, deep, 6, around, radial), f32),
            dma((4,)),
            dma((ITERS, 4)),
            dma((ITERS, 4)),
            dma((ITERS, 2)),
            dma((ITERS, 2)),
            dma((ITERS, across)),
            dma((ITERS, across)),
            dma((ITERS, deep)),
            dma((ITERS, deep)),
        ],
        compiler_params=pltpu.CompilerParams(collective_id=turn, has_side_effects=True),
        name="sweeps",
    )(*args)


OUT = pltpu.VMEM


def put_kernel(first_ref, second_ref, first_out, second_out, sems):
    copies = (
        pltpu.make_async_copy(first_ref, first_out, sems.at[0]),
        pltpu.make_async_copy(second_ref, second_out, sems.at[1]),
    )
    for copy in copies:
        copy.start()
    for copy in copies:
        copy.wait()


def put(*values):
    anywhere = pl.BlockSpec(memory_space=pl.ANY)
    return pl.pallas_call(
        put_kernel,
        out_shape=[jax.ShapeDtypeStruct(value.shape, value.dtype) for value in values],
        in_specs=[anywhere] * 2,
        out_specs=[anywhere] * 2,
        scratch_shapes=[pltpu.SemaphoreType.DMA((2,))],
        name="put",
    )(*values)


def shards(prev, source, faces, inverse, sector_offset, donor_cells, donor_weights):
    sectors = lax.axis_size("sector")
    along = radices(sectors)[2]
    branches = [functools.partial(swept, turn, sectors, lax.axis_size("block")) for turn in range(along)]
    result = lax.switch(
        lax.rem(sector_offset[0], along),
        branches,
        prev,
        source,
        faces,
        inverse,
        sector_offset,
        donor_cells,
        donor_weights,
    )
    return tuple(result)


def solution(mesh):
    return jax.shard_map(
        shards,
        mesh=mesh,
        in_specs=(
            P(None, "block", "sector", None),
            P(None, "block", "sector", None),
            P(None, None, None, "block", "sector", None),
            P(None, None, "block", "sector", None),
            P(),
            P("sector"),
            P("sector"),
        ),
        out_specs=(P(None, "block", "sector", None), P(None, "block", "sector", None)),
        check_vma=False,
    )
```
